32 devices in a mesh: pair: 1 (over z), tp: 4 (over y), side: 8 (over x, core).
Axes of the slice: x: 4, y: 4, z: 1, core: 2. Of those that a mesh axis runs over, the one named last changes fastest.
The devices are a block of a 4x4x8 slice.
Arguments:
- x_prompt: bfloat16 [4096, 4096], P(('pair', 'side'))
- s_len: int32 [8], P(('pair', 'side'))
- y_tok: bfloat16 [64, 4096], P(('pair', 'side'))
- k_cache: bfloat16 [1, 64, 768, 2, 4, 128], P(None, ('pair', 'side'), None, None, 'tp')
- v_cache: bfloat16 [1, 64, 768, 2, 4, 128], P(None, ('pair', 'side'), None, None, 'tp')
- c_len: int32 [64], P(('pair', 'side'))
- wqkv_a: bfloat16 [1, 4096, 8, 768], P(None, None, 'tp')
- wo_a: bfloat16 [1, 8, 512, 4096], P(None, 'tp')
- wug_a: bfloat16 [1, 4096, 2, 14336], P(None, None, None, 'tp')
- wd_a: bfloat16 [1, 14336, 4096], P(None, 'tp')
- norm_a: bfloat16 [1, 2, 4096], replicated
- wqkv_b: bfloat16 [1, 4096, 2, 4, 768], P(None, None, None, 'tp')
- wo_b: bfloat16 [1, 2, 4, 512, 4096], P(None, None, 'tp')
- wug_b: bfloat16 [1, 4096, 2, 14336], P(None, None, None, 'tp')
- wd_b: bfloat16 [1, 14336, 4096], P(None, 'tp')
- norm_b: bfloat16 [1, 2, 4096], replicated
Outputs:
- output 1: bfloat16 [4096, 4096], P(('pair', 'side'))
- output 2: bfloat16 [64, 4096], P(('pair', 'side'))
- output 3: bfloat16 [1, 4096, 2, 4, 128], P(None, ('pair', 'side'), None, 'tp')
- output 4: bfloat16 [1, 4096, 2, 4, 128], P(None, ('pair', 'side'), None, 'tp')
- output 5: bfloat16 [1, 64, 768, 2, 4, 128], P(None, ('pair', 'side'), None, None, 'tp')
- output 6: bfloat16 [1, 64, 768, 2, 4, 128], P(None, ('pair', 'side'), None, None, 'tp')
All inputs are finite; a program needn't handle non-finite values.
Results may differ from the reference program's by a relative error of at most 0.0075918.
Values are sent between devices in bfloat16 or wider.
A program may use at most 768 MiB of HBM per device.

```python
import jax
import jax.numpy as jnp
from jax import lax

PROMPT = 512
DMODEL = 4096
Q_HEADS = 32
KV_HEADS = 8
HEAD_DIM = 128
FFN_DIM = 14336
LAYERS = 1
DEC_BATCH = 8
CACHE_LEN = 768
TP_SIZE = 4
NUM_SIDES = 8
KV_LOCAL = KV_HEADS // TP_SIZE
Q_GROUP = Q_HEADS // KV_HEADS
QKV_WIDTH = (Q_GROUP + 2) * HEAD_DIM
ROPE_BASE = 10000.0
NORM_EPS = 1e-5


def setup_inputs(seed: int = 0, part: int = 0) -> dict:
    weight_key, part_key = jax.random.split(jax.random.key(seed))
    wkeys = jax.random.split(weight_key, 10)
    pkeys = jax.random.split(jax.random.fold_in(part_key, part), 8)
    prompt_rows = NUM_SIDES * PROMPT
    batch_rows = NUM_SIDES * DEC_BATCH
    cache_shape = (LAYERS, batch_rows, CACHE_LEN, KV_LOCAL, TP_SIZE, HEAD_DIM)

    def normal_w(rkey, shape, fan_in):
        return (jax.random.normal(rkey, shape, jnp.float32) * fan_in ** -0.5).astype(jnp.bfloat16)

    def gain_draw(rkey):
        return (0.5 + jax.random.uniform(rkey, (LAYERS, 2, DMODEL), jnp.float32)).astype(jnp.bfloat16)

    lens_raw = jax.random.randint(pkeys[1], (NUM_SIDES,), 3 * PROMPT // 4, PROMPT + 1)
    full_at = jax.random.randint(pkeys[2], (), 0, NUM_SIDES)
    s_len = jnp.where(jnp.arange(NUM_SIDES) == full_at, PROMPT, lens_raw).astype(jnp.int32)
    ctx_raw = jax.random.randint(pkeys[6], (batch_rows,), CACHE_LEN // 2, CACHE_LEN)
    long_at = jax.random.randint(pkeys[7], (), 0, batch_rows)
    c_len = jnp.where(jnp.arange(batch_rows) == long_at, CACHE_LEN - 1, ctx_raw).astype(jnp.int32)
    return {
        'x_prompt': jax.random.normal(pkeys[0], (prompt_rows, DMODEL), jnp.float32).astype(jnp.bfloat16),
        's_len': s_len,
        'y_tok': jax.random.normal(pkeys[3], (batch_rows, DMODEL), jnp.float32).astype(jnp.bfloat16),
        'k_cache': jax.random.normal(pkeys[4], cache_shape, jnp.float32).astype(jnp.bfloat16),
        'v_cache': jax.random.normal(pkeys[5], cache_shape, jnp.float32).astype(jnp.bfloat16),
        'c_len': c_len,
        'wqkv_a': normal_w(wkeys[0], (LAYERS, DMODEL, KV_HEADS, QKV_WIDTH), DMODEL),
        'wo_a': normal_w(wkeys[1], (LAYERS, KV_HEADS, Q_GROUP * HEAD_DIM, DMODEL), Q_HEADS * HEAD_DIM),
        'wug_a': normal_w(wkeys[2], (LAYERS, DMODEL, 2, FFN_DIM), DMODEL),
        'wd_a': normal_w(wkeys[3], (LAYERS, FFN_DIM, DMODEL), FFN_DIM),
        'norm_a': gain_draw(wkeys[4]),
        'wqkv_b': normal_w(wkeys[5], (LAYERS, DMODEL, KV_LOCAL, TP_SIZE, QKV_WIDTH), DMODEL),
        'wo_b': normal_w(wkeys[6], (LAYERS, KV_LOCAL, TP_SIZE, Q_GROUP * HEAD_DIM, DMODEL), Q_HEADS * HEAD_DIM),
        'wug_b': normal_w(wkeys[7], (LAYERS, DMODEL, 2, FFN_DIM), DMODEL),
        'wd_b': normal_w(wkeys[8], (LAYERS, FFN_DIM, DMODEL), FFN_DIM),
        'norm_b': gain_draw(wkeys[9]),
    }


def rms_norm(hidden, gain):
    val_f32 = hidden.astype(jnp.float32)
    inv_rms = lax.rsqrt(jnp.mean(val_f32 * val_f32, axis=-1, keepdims=True) + NORM_EPS)
    return (val_f32 * inv_rms * gain.astype(jnp.float32)).astype(jnp.bfloat16)


def rope_rot(vals_in, positions):
    half_dim = vals_in.shape[-1] // 2
    inv_freq = ROPE_BASE ** (-jnp.arange(half_dim, dtype=jnp.float32) / half_dim)
    angles = positions.astype(jnp.float32)[:, None] * inv_freq[None, :]
    tab_shape = (angles.shape[0],) + (1,) * (vals_in.ndim - 2) + (half_dim,)
    cos_tab = jnp.cos(angles).reshape(tab_shape)
    sin_tab = jnp.sin(angles).reshape(tab_shape)
    lo_half = vals_in[..., :half_dim].astype(jnp.float32)
    hi_half = vals_in[..., half_dim:].astype(jnp.float32)
    return jnp.concatenate([lo_half * cos_tab - hi_half * sin_tab, hi_half * cos_tab + lo_half * sin_tab], axis=-1).astype(jnp.bfloat16)


def mlp_block(hidden, w_ug, w_down, gain):
    normed = rms_norm(hidden, gain)
    upgate = jnp.dot(normed, w_ug.reshape(DMODEL, 2 * FFN_DIM), preferred_element_type=jnp.float32).astype(jnp.bfloat16)
    upgate = upgate.reshape(hidden.shape[0], 2, FFN_DIM)
    act_out = (jax.nn.silu(upgate[:, 1].astype(jnp.float32)) * upgate[:, 0].astype(jnp.float32)).astype(jnp.bfloat16)
    mlp_down = jnp.dot(act_out, w_down, preferred_element_type=jnp.float32).astype(jnp.bfloat16)
    return (hidden.astype(jnp.float32) + mlp_down.astype(jnp.float32)).astype(jnp.bfloat16)


def prompt_layer(hidden, q_start, prev_k, prev_v, seq_len, w_qkv, w_out, w_ug, w_down, gain_pair):
    num_rows = hidden.shape[0]
    positions = q_start + jnp.arange(num_rows)
    normed = rms_norm(hidden, gain_pair[0])
    qkv_all = jnp.dot(normed, w_qkv.reshape(DMODEL, KV_HEADS * QKV_WIDTH), preferred_element_type=jnp.float32).astype(jnp.bfloat16)
    qkv_all = qkv_all.reshape(num_rows, KV_HEADS, Q_GROUP + 2, HEAD_DIM)
    queries = rope_rot(qkv_all[:, :, :Q_GROUP], positions)
    key_new = rope_rot(qkv_all[:, :, Q_GROUP], positions)
    val_new = qkv_all[:, :, Q_GROUP + 1]
    key_all = jnp.concatenate([prev_k, key_new], axis=0)
    val_all = jnp.concatenate([prev_v, val_new], axis=0)
    key_pos = jnp.arange(q_start + num_rows)
    allowed = (key_pos[None, :] <= positions[:, None]) & (key_pos[None, :] < seq_len)

    def head_attention(packed):
        q_head, k_head, v_head = packed
        scores = jnp.einsum('qgd,kd->gqk', q_head.astype(jnp.float32), k_head.astype(jnp.float32)) * HEAD_DIM ** -0.5
        scores = jnp.where(allowed[None], scores, -1e30)
        attn_prob = jax.nn.softmax(scores, axis=-1).astype(jnp.bfloat16)
        return jnp.einsum('gqk,kd->qgd', attn_prob.astype(jnp.float32), v_head.astype(jnp.float32)).astype(jnp.bfloat16)

    attn_out = lax.map(head_attention, (jnp.transpose(queries, (1, 0, 2, 3)), jnp.transpose(key_all, (1, 0, 2)), jnp.transpose(val_all, (1, 0, 2))))
    attn_out = jnp.transpose(attn_out, (1, 0, 2, 3)).reshape(num_rows, Q_HEADS * HEAD_DIM)
    attn_proj = jnp.dot(attn_out, w_out.reshape(Q_HEADS * HEAD_DIM, DMODEL), preferred_element_type=jnp.float32).astype(jnp.bfloat16)
    hidden = (hidden.astype(jnp.float32) + attn_proj.astype(jnp.float32)).astype(jnp.bfloat16)
    hidden = mlp_block(hidden, w_ug, w_down, gain_pair[1])
    return hidden, key_new, val_new


def prefill_side(x_rows, seq_len, wqkv_a, wo_a, wug_a, wd_a, norm_a):
    half_len = PROMPT // 2
    no_prev = jnp.zeros((0, KV_HEADS, HEAD_DIM), jnp.bfloat16)

    def first_step(hidden, layer_w):
        w_qkv, w_out, w_ug, w_down, gain_pair = layer_w
        hidden, key_new, val_new = prompt_layer(hidden, 0, no_prev, no_prev, seq_len, w_qkv, w_out, w_ug, w_down, gain_pair)
        return hidden, (key_new, val_new)

    def second_step(hidden, layer_w):
        w_qkv, w_out, w_ug, w_down, gain_pair, prev_k, prev_v = layer_w
        hidden, key_new, val_new = prompt_layer(hidden, half_len, prev_k, prev_v, seq_len, w_qkv, w_out, w_ug, w_down, gain_pair)
        return hidden, (key_new, val_new)

    weights = (wqkv_a, wo_a, wug_a, wd_a, norm_a)
    hidden_first, (keys_first, vals_first) = lax.scan(first_step, x_rows[:half_len], weights)
    hidden_second, (keys_second, vals_second) = lax.scan(second_step, x_rows[half_len:], weights + (keys_first, vals_first))
    valid = (jnp.arange(PROMPT) < seq_len)[None, :, None, None]
    key_cache = jnp.where(valid, jnp.concatenate([keys_first, keys_second], axis=1), 0.0).astype(jnp.bfloat16)
    val_cache = jnp.where(valid, jnp.concatenate([vals_first, vals_second], axis=1), 0.0).astype(jnp.bfloat16)
    return jnp.concatenate([hidden_first, hidden_second], axis=0), key_cache, val_cache


def decode_side(tokens, lengths, k_cache, v_cache, wqkv_b, wo_b, wug_b, wd_b, norm_b):
    slot_pos = jnp.arange(CACHE_LEN)
    write_slot = (slot_pos[None, :] == lengths[:, None])[:, :, None, None]

    def row_attention(packed):
        q_row, k_row, v_row, len_row = packed
        scores = jnp.einsum('hgd,thd->hgt', q_row.astype(jnp.float32), k_row.astype(jnp.float32)) * HEAD_DIM ** -0.5
        scores = jnp.where((slot_pos <= len_row)[None, None, :], scores, -1e30)
        attn_prob = jax.nn.softmax(scores, axis=-1).astype(jnp.bfloat16)
        return jnp.einsum('hgt,thd->hgd', attn_prob.astype(jnp.float32), v_row.astype(jnp.float32)).astype(jnp.bfloat16)

    def layer_step(hidden, layer_w):
        w_qkv, w_out, w_ug, w_down, gain_pair, cache_k, cache_v = layer_w
        normed = rms_norm(hidden, gain_pair[0])
        qkv_all = jnp.dot(normed, w_qkv.reshape(DMODEL, KV_HEADS * QKV_WIDTH), preferred_element_type=jnp.float32).astype(jnp.bfloat16)
        qkv_all = qkv_all.reshape(DEC_BATCH, KV_HEADS, Q_GROUP + 2, HEAD_DIM)
        queries = rope_rot(qkv_all[:, :, :Q_GROUP], lengths)
        key_new = rope_rot(qkv_all[:, :, Q_GROUP], lengths)
        val_new = qkv_all[:, :, Q_GROUP + 1]
        key_upd = jnp.where(write_slot, key_new[:, None], cache_k)
        val_upd = jnp.where(write_slot, val_new[:, None], cache_v)
        attn_out = lax.map(row_attention, (queries, key_upd, val_upd, lengths))
        attn_proj = jnp.dot(attn_out.reshape(DEC_BATCH, Q_HEADS * HEAD_DIM), w_out.reshape(Q_HEADS * HEAD_DIM, DMODEL), preferred_element_type=jnp.float32).astype(jnp.bfloat16)
        hidden = (hidden.astype(jnp.float32) + attn_proj.astype(jnp.float32)).astype(jnp.bfloat16)
        hidden = mlp_block(hidden, w_ug, w_down, gain_pair[1])
        return hidden, (key_upd, val_upd)

    hidden, (k_new, v_new) = lax.scan(layer_step, tokens, (wqkv_b, wo_b, wug_b, wd_b, norm_b, k_cache, v_cache))
    return hidden, k_new, v_new


def reference(x_prompt, s_len, y_tok, k_cache, v_cache, c_len, wqkv_a, wo_a, wug_a, wd_a, norm_a, wqkv_b, wo_b, wug_b, wd_b, norm_b):
    def one_prefill(packed):
        x_rows, seq_len = packed
        return prefill_side(x_rows, seq_len, wqkv_a, wo_a, wug_a, wd_a, norm_a)

    hidden_all, keys_all, vals_all = lax.map(one_prefill, (x_prompt.reshape(NUM_SIDES, PROMPT, DMODEL), s_len))

    def install(cache_all):
        moved = jnp.roll(cache_all, NUM_SIDES // 2, axis=0)
        return jnp.transpose(moved, (1, 0, 2, 3, 4)).reshape(LAYERS, NUM_SIDES * PROMPT, KV_LOCAL, TP_SIZE, HEAD_DIM)

    side_shape = (LAYERS, NUM_SIDES, DEC_BATCH, CACHE_LEN, KV_HEADS, HEAD_DIM)
    k_sides = jnp.transpose(k_cache.reshape(side_shape), (1, 0, 2, 3, 4, 5))
    v_sides = jnp.transpose(v_cache.reshape(side_shape), (1, 0, 2, 3, 4, 5))

    def one_decode(packed):
        tokens, lengths, cache_k, cache_v = packed
        return decode_side(tokens, lengths, cache_k, cache_v, wqkv_b, wo_b, wug_b, wd_b, norm_b)

    y_sides, k_new, v_new = lax.map(one_decode, (y_tok.reshape(NUM_SIDES, DEC_BATCH, DMODEL), c_len.reshape(NUM_SIDES, DEC_BATCH), k_sides, v_sides))
    out_shape = (LAYERS, NUM_SIDES * DEC_BATCH, CACHE_LEN, KV_LOCAL, TP_SIZE, HEAD_DIM)
    k_out = jnp.transpose(k_new, (1, 0, 2, 3, 4, 5)).reshape(out_shape)
    v_out = jnp.transpose(v_new, (1, 0, 2, 3, 4, 5)).reshape(out_shape)
    return (hidden_all.reshape(NUM_SIDES * PROMPT, DMODEL), y_sides.reshape(NUM_SIDES * DEC_BATCH, DMODEL), install(keys_all), install(vals_all), k_out, v_out)
```

```python
import jax
import jax.numpy as jnp
from jax import lax
from jax.experimental import pallas as pl
from jax.experimental.pallas import tpu as pltpu
from jax.sharding import PartitionSpec as P

ROPE_BASE = 10000.0
NORM_EPS = 1e-5
F32 = jnp.float32
BF16 = jnp.bfloat16


def rms_norm(hidden, gain):
    val_f32 = hidden.astype(F32)
    inv_rms = lax.rsqrt(jnp.mean(val_f32 * val_f32, axis=-1, keepdims=True) + NORM_EPS)
    return (val_f32 * inv_rms * gain.astype(F32)).astype(BF16)


def rope_rot(vals_in, positions):
    half_dim = vals_in.shape[-1] // 2
    inv_freq = ROPE_BASE ** (-jnp.arange(half_dim, dtype=F32) / half_dim)
    angles = positions.astype(F32)[:, None] * inv_freq[None, :]
    tab_shape = (angles.shape[0],) + (1,) * (vals_in.ndim - 2) + (half_dim,)
    cos_tab = jnp.cos(angles).reshape(tab_shape)
    sin_tab = jnp.sin(angles).reshape(tab_shape)
    lo_half = vals_in[..., :half_dim].astype(F32)
    hi_half = vals_in[..., half_dim:].astype(F32)
    return jnp.concatenate([lo_half * cos_tab - hi_half * sin_tab, hi_half * cos_tab + lo_half * sin_tab], axis=-1).astype(BF16)


def residual(hidden, delta_f32):
    return (hidden.astype(F32) + delta_f32.astype(BF16).astype(F32)).astype(BF16)


def up_act(normed, w_ug):
    upgate = jnp.einsum('sd,dkf->skf', normed, w_ug, preferred_element_type=F32).astype(BF16)
    return (jax.nn.silu(upgate[:, 1].astype(F32)) * upgate[:, 0].astype(F32)).astype(BF16)


def ring_maps(tp_size):
    fwd = [(i, (i + 1) % tp_size) for i in range(tp_size)]
    bwd = [(i, (i - 1) % tp_size) for i in range(tp_size)]
    return fwd, bwd


def ring_reduce_scatter(part, tp_size):
    fwd, bwd = ring_maps(tp_size)
    rows = part.shape[0] // tp_size
    half = rows // 2
    blk = [part[j * rows:(j + 1) * rows] for j in range(tp_size)]
    got_f = lax.ppermute(jnp.concatenate([blk[2][:half], blk[1][half:]]), 'tp', fwd)
    got_b = lax.ppermute(jnp.concatenate([blk[3][:half], blk[2][half:]]), 'tp', bwd)
    last_f = lax.ppermute(blk[1][:half] + got_f[:half], 'tp', fwd)
    last_b = lax.ppermute(blk[3][half:] + got_b[half:], 'tp', bwd)
    top = blk[0][:half] + (last_f + got_b[:half])
    bot = blk[0][half:] + (got_f[half:] + last_b)
    return jnp.concatenate([top, bot])


def ring_all_gather(own, tp_size):
    fwd, bwd = ring_maps(tp_size)
    half = own.shape[0] // 2
    prev_blk = lax.ppermute(own, 'tp', fwd)
    next_blk = lax.ppermute(own, 'tp', bwd)
    far_top = lax.ppermute(prev_blk[:half], 'tp', fwd)
    far_bot = lax.ppermute(next_blk[half:], 'tp', bwd)
    return [own, next_blk, jnp.concatenate([far_top, far_bot]), prev_blk]


def roll_rows(vals, start):
    return lax.dynamic_slice_in_dim(jnp.concatenate([vals, vals]), start, vals.shape[0], axis=0)


def prompt_attention(x_rows, seq_len, w_qkv, head_dim, group, gain, half_len):
    num_rows = x_rows.shape[0]
    kv_loc = w_qkv.shape[1]
    positions = jnp.arange(num_rows)
    normed = rms_norm(x_rows, gain)
    qkv_all = jnp.einsum('sd,dhe->she', normed, w_qkv, preferred_element_type=F32).astype(BF16)
    qkv_all = qkv_all.reshape(num_rows, kv_loc, group + 2, head_dim)
    queries = rope_rot(qkv_all[:, :, :group], positions)
    key_all = rope_rot(qkv_all[:, :, group], positions)
    val_all = qkv_all[:, :, group + 1]
    outs = []
    for q_start in range(0, num_rows, half_len):
        k_end = q_start + half_len
        key_pos = jnp.arange(k_end)
        allowed = (key_pos[None, :] <= positions[q_start:k_end, None]) & (key_pos[None, :] < seq_len)
        scores = jnp.einsum('qhgd,khd->hgqk', queries[q_start:k_end], key_all[:k_end], preferred_element_type=F32) * head_dim ** -0.5
        scores = jnp.where(allowed, scores, -1e30)
        attn_prob = jax.nn.softmax(scores, axis=-1).astype(BF16)
        attn_out = jnp.einsum('hgqk,khd->qhgd', attn_prob, val_all[:k_end], preferred_element_type=F32).astype(BF16)
        outs.append(attn_out.reshape(half_len, kv_loc * group * head_dim))
    valid = (positions < seq_len)[:, None, None]
    zero_val = jnp.zeros((), BF16)
    return outs, jnp.where(valid, key_all, zero_val), jnp.where(valid, val_all, zero_val)


def hand_off(key_cache, val_cache, tp_size, side_size):
    t_idx = lax.axis_index('tp')
    both = jnp.stack([key_cache, val_cache])
    head0, head1 = both[:, :, 0], both[:, :, 1]
    low = t_idx < tp_size // 2
    received = []
    for rnd in range(2):
        piece = jnp.where(low, head1, head0) if rnd else jnp.where(low, head0, head1)
        pairs = []
        for t in range(tp_size):
            for s in range(side_size):
                dst_t = (t % 2) * 2 + (rnd + t // 2) % 2
                pairs.append((t * side_size + s, dst_t * side_size + (s + side_size // 2) % side_size))
        received.append(lax.ppermute(piece, ('tp', 'side'), pairs))
    even = t_idx % 2 == 0
    slot0 = jnp.where(even, received[0], received[1])
    slot1 = jnp.where(even, received[1], received[0])
    out = jnp.stack([slot0, slot1], axis=2)
    return out[0][None, :, :, None], out[1][None, :, :, None]


def cache_kernel(len_ref, kc_ref, vc_ref, kn_ref, vn_ref, ko_ref, vo_ref):
    slot = len_ref[pl.program_id(0)]
    ko_ref[...] = kc_ref[...]
    vo_ref[...] = vc_ref[...]
    ko_ref[0, pl.ds(slot, 1)] = kn_ref[...]
    vo_ref[0, pl.ds(slot, 1)] = vn_ref[...]


def cache_update(lengths, k_cache, v_cache, key_new, val_new):
    rows, slots, kv_loc, dim = k_cache.shape
    big = pl.BlockSpec((1, slots, kv_loc, dim), lambda b, lens: (b, 0, 0, 0))
    small = pl.BlockSpec((1, kv_loc, dim), lambda b, lens: (b, 0, 0))
    shape = jax.ShapeDtypeStruct(k_cache.shape, k_cache.dtype)
    return pl.pallas_call(
        cache_kernel,
        grid_spec=pltpu.PrefetchScalarGridSpec(num_scalar_prefetch=1, grid=(rows,), in_specs=[big, big, small, small], out_specs=[big, big]),
        out_shape=[shape, shape],
        cost_estimate=pl.CostEstimate(flops=10 ** 9, bytes_accessed=4 * k_cache.size * 2, transcendentals=0),
        name='cache_update',
    )(lengths, k_cache, v_cache, key_new, val_new)


def decode_side(tokens, lengths, k_cache, v_cache, w_qkv, w_out, w_ug, w_down, gains):
    batch_rows = tokens.shape[0]
    kv_loc = w_qkv.shape[1]
    head_dim = (w_qkv.shape[2] - w_out.shape[1]) // 2
    group = w_out.shape[1] // head_dim
    visible = (jnp.arange(k_cache.shape[1])[None, :] <= lengths[:, None])[:, None, None, :]
    normed = rms_norm(tokens, gains[0])
    qkv_all = jnp.einsum('bd,die->bie', normed, w_qkv, preferred_element_type=F32).astype(BF16)
    qkv_all = qkv_all.reshape(batch_rows, kv_loc, group + 2, head_dim)
    queries = rope_rot(qkv_all[:, :, :group], lengths)
    key_new = rope_rot(qkv_all[:, :, group], lengths)
    val_new = qkv_all[:, :, group + 1]
    key_upd, val_upd = cache_update(lengths, k_cache, v_cache, key_new, val_new)
    scores = jnp.einsum('bige,bsie->bigs', queries, key_upd, preferred_element_type=F32) * head_dim ** -0.5
    scores = jnp.where(visible, scores, -1e30)
    attn_prob = jax.nn.softmax(scores, axis=-1).astype(BF16)
    attn_out = jnp.einsum('bigs,bsie->bige', attn_prob, val_upd, preferred_element_type=F32).astype(BF16)
    attn_proj = lax.psum(jnp.einsum('bif,ifd->bd', attn_out.reshape(batch_rows, kv_loc, group * head_dim), w_out, preferred_element_type=F32), 'tp')
    hidden = residual(tokens, attn_proj)
    act = up_act(rms_norm(hidden, gains[1]), w_ug)
    hidden = residual(hidden, lax.psum(jnp.dot(act, w_down, preferred_element_type=F32), 'tp'))
    return hidden, key_upd, val_upd


def solution(mesh):
    tp_size = mesh.shape['tp']
    side_size = mesh.shape['side']
    rows_spec = P(('pair', 'side'), None)
    flat_spec = P(('pair', 'side'))
    cache_spec = P(None, ('pair', 'side'), None, None, 'tp', None)
    prompt_spec = P(None, ('pair', 'side'), None, 'tp', None)
    in_specs = (rows_spec, flat_spec, rows_spec, cache_spec, cache_spec, flat_spec,
                P(None, None, 'tp', None), P(None, 'tp', None, None), P(None, None, None, 'tp'), P(None, 'tp', None), P(),
                P(None, None, None, 'tp', None), P(None, None, 'tp', None, None), P(None, None, None, 'tp'), P(None, 'tp', None), P())
    out_specs = (rows_spec, rows_spec, prompt_spec, prompt_spec, cache_spec, cache_spec)

    def body(x_prompt, s_len, y_tok, k_cache, v_cache, c_len, wqkv_a, wo_a, wug_a, wd_a, norm_a, wqkv_b, wo_b, wug_b, wd_b, norm_b):
        t_idx = lax.axis_index('tp')
        half_len = x_prompt.shape[0] // 2
        blk = half_len // tp_size
        head_dim = (wqkv_a.shape[3] - wo_a.shape[2]) // 2
        group = wo_a.shape[2] // head_dim
        w_out = wo_a[0].reshape(-1, wo_a.shape[3])
        attn, key_cache, val_cache = prompt_attention(x_prompt, s_len[0], wqkv_a[0], head_dim, group, norm_a[0, 0], half_len)
        own_h, normed = [], []
        for idx in range(2):
            part = jnp.dot(roll_rows(attn[idx], t_idx * blk), w_out, preferred_element_type=F32)
            own = lax.dynamic_slice_in_dim(x_prompt, idx * half_len + t_idx * blk, blk, axis=0)
            own = residual(own, ring_reduce_scatter(part, tp_size))
            own_h.append(own)
            normed.append(jnp.concatenate(ring_all_gather(rms_norm(own, norm_a[0, 1]), tp_size)))
        k_prompt, v_prompt = hand_off(key_cache, val_cache, tp_size, side_size)
        hidden = jnp.zeros_like(x_prompt)
        for idx in range(2):
            act = up_act(normed[idx], wug_a[0])
            part = jnp.dot(act, wd_a[0], preferred_element_type=F32)
            own = residual(own_h[idx], ring_reduce_scatter(part, tp_size))
            for j, rows in enumerate(ring_all_gather(own, tp_size)):
                hidden = lax.dynamic_update_slice_in_dim(hidden, rows, idx * half_len + lax.rem(t_idx + j, tp_size) * blk, axis=0)
        kc = k_cache[0, :, :, :, 0]
        vc = v_cache[0, :, :, :, 0]
        y_out, k_new, v_new = decode_side(y_tok, c_len, kc, vc, wqkv_b[0, :, :, 0], wo_b[0, :, 0], wug_b[0], wd_b[0], norm_b[0])
        return hidden, y_out, k_prompt, v_prompt, k_new[None, :, :, :, None], v_new[None, :, :, :, None]

    return jax.shard_map(body, mesh=mesh, in_specs=in_specs, out_specs=out_specs, check_vma=False)
```

```python
import jax
import jax.numpy as jnp
from jax import lax
from jax.experimental import pallas as pl
from jax.experimental.pallas import tpu as pltpu
from jax.sharding import PartitionSpec as P

ROPE_BASE = 10000.0
NORM_EPS = 1e-5
F32 = jnp.float32
BF16 = jnp.bfloat16


def rms_norm(hidden, gain):
    val_f32 = hidden.astype(F32)
    inv_rms = lax.rsqrt(jnp.mean(val_f32 * val_f32, axis=-1, keepdims=True) + NORM_EPS)
    return (val_f32 * inv_rms * gain.astype(F32)).astype(BF16)


def rope_rot(vals_in, positions):
    half_dim = vals_in.shape[-1] // 2
    inv_freq = ROPE_BASE ** (-jnp.arange(half_dim, dtype=F32) / half_dim)
    angles = positions.astype(F32)[:, None] * inv_freq[None, :]
    tab_shape = (angles.shape[0],) + (1,) * (vals_in.ndim - 2) + (half_dim,)
    cos_tab = jnp.cos(angles).reshape(tab_shape)
    sin_tab = jnp.sin(angles).reshape(tab_shape)
    lo_half = vals_in[..., :half_dim].astype(F32)
    hi_half = vals_in[..., half_dim:].astype(F32)
    return jnp.concatenate([lo_half * cos_tab - hi_half * sin_tab, hi_half * cos_tab + lo_half * sin_tab], axis=-1).astype(BF16)


def residual(hidden, delta_f32):
    return (hidden.astype(F32) + delta_f32.astype(BF16).astype(F32)).astype(BF16)


def up_act(normed, w_ug):
    upgate = jnp.einsum('sd,dkf->skf', normed, w_ug, preferred_element_type=F32).astype(BF16)
    return (jax.nn.silu(upgate[:, 1].astype(F32)) * upgate[:, 0].astype(F32)).astype(BF16)


MESH = pl.DeviceIdType.MESH
SUB = 512


def mega_kernel(attn, xown, gain, wo_hbm, wug_hbm, wd_hbm, out_hbm, dense_hbm,
                part, r1, r2, nfull, hown, act, wbuf, dbuf, raw, f32s,
                s1_send, s1_recv, s2_send, s2_recv, ag_send, ag_recv,
                w_sem, d_sem, raw_sem, put_sem, out_sem):
    tp_size = lax.axis_size('tp')
    me = lax.axis_index('tp')
    right, left = lax.rem(me + 1, tp_size), lax.rem(me + tp_size - 1, tp_size)
    _, n_grp, rows, width = part.shape
    blk = rows // tp_size
    half = blk // 2
    depth = wug_hbm.shape[0]
    n_tile = dense_hbm.shape[0]
    n_up = n_tile // 2
    n_down = wd_hbm.shape[1] // SUB
    k_out = wo_hbm.shape[0]
    peers = (right, left)

    barrier = pltpu.get_barrier_semaphore()
    for peer in peers:
        pl.semaphore_signal(barrier, inc=1, device_id={'tp': peer}, device_id_type=MESH)
    pl.semaphore_wait(barrier, 2)

    def remote(src, dst, send, recv, way):
        return pltpu.make_async_remote_copy(src_ref=src, dst_ref=dst, send_sem=send, recv_sem=recv,
                                            device_id={'tp': peers[way]}, device_id_type=MESH)

    def s1_copy(st, h, g, way):
        src = part.at[h, g, pl.ds(blk + half + way * blk, blk)]
        return remote(src, r1.at[st, h, way, g], s1_send.at[st, h, way, g], s1_recv.at[st, h, way, g], way)

    def s2_copy(st, h, g, way):
        src = part.at[h, g, pl.ds(blk if way == 0 else 3 * blk + half, half)]
        return remote(src, r2.at[st, h, way, g], s2_send.at[st, h, way, g], s2_recv.at[st, h, way, g], way)

    def ag1_copy(st, h, way):
        return remote(nfull.at[h, pl.ds(0, blk)], nfull.at[h, pl.ds(3 * blk if way == 0 else blk, blk)],
                      ag_send.at[st, h, way, 0], ag_recv.at[st, h, way, 0], way)

    def ag2_copy(st, h, way):
        src = nfull.at[h, pl.ds(3 * blk if way == 0 else blk + half, half)]
        return remote(src, nfull.at[h, pl.ds(2 * blk + way * half, half)],
                      ag_send.at[st, h, way, 1], ag_recv.at[st, h, way, 1], way)

    def send_s1(st, h, g):
        for way in range(2):
            s1_copy(st, h, g, way).start()

    def ev_s2(st, h, g):
        for way in range(2):
            s1_copy(st, h, g, way).wait_recv()
        part[h, g, blk:blk + half] += r1[st, h, 0, g, half:]
        s2_copy(st, h, g, 0).start()
        part[h, g, 3 * blk + half:] += r1[st, h, 1, g, :half]
        s2_copy(st, h, g, 1).start()

    def ev_final(st, h):
        for g in range(n_grp):
            for way in range(2):
                s2_copy(st, h, g, way).wait_recv()
            cols = slice(g * width, (g + 1) * width)
            base = xown if st == 0 else hown
            top = part[h, g, :half] + (r1[st, h, 1, g, half:] + r2[st, h, 0, g])
            bot = part[h, g, half:blk] + (r1[st, h, 0, g, :half] + r2[st, h, 1, g])
            total = jnp.concatenate([top, bot], axis=0).astype(BF16)
            new = (base[h, :, cols].astype(F32) + total.astype(F32)).astype(BF16)
            if st == 0:
                hown[h, :, cols] = new
            else:
                nfull[h, :blk, cols] = new
        if st == 0:
            for r in range(0, blk, 16):
                val = hown[h, r:r + 16].astype(F32)
                inv = lax.rsqrt(jnp.mean(val * val, axis=-1, keepdims=True) + NORM_EPS)
                nfull[h, r:r + 16] = (val * inv * gain[...].astype(F32)).astype(BF16)
        for way in range(2):
            ag1_copy(st, h, way).start()

    def ev_ag2(st, h):
        for way in range(2):
            ag1_copy(st, h, way).wait_recv()
            ag2_copy(st, h, way).start()

    def ev_ag_done(st, h):
        for way in range(2):
            ag2_copy(st, h, way).wait_recv()

    def drain(st, h):
        for way in range(2):
            for g in range(n_grp):
                s1_copy(st, h, g, way).wait_send()
                s2_copy(st, h, g, way).wait_send()
            ag1_copy(st, h, way).wait_send()
            ag2_copy(st, h, way).wait_send()

    def wo_load(c, slot):
        return pltpu.make_async_copy(wo_hbm.at[:, pl.ds(pl.multiple_of(c * SUB, SUB), SUB)], dbuf.at[slot, pl.ds(0, k_out)], d_sem.at[slot])

    def wd_load(c, slot):
        return pltpu.make_async_copy(wd_hbm.at[:, pl.ds(pl.multiple_of(c * SUB, SUB), SUB)], dbuf.at[slot], d_sem.at[slot])

    def raw_load(i, slot):
        return pltpu.make_async_copy(wug_hbm.at[:, :, pl.ds(pl.multiple_of(i * 128, 128), 128)], raw.at[slot], raw_sem.at[slot])

    def put_store(i, slot):
        return pltpu.make_async_copy(wbuf.at[slot, 0], dense_hbm.at[i], put_sem.at[slot])

    def up_load(c, slot):
        return pltpu.make_async_copy(dense_hbm.at[pl.ds(2 * c, 2)], wbuf.at[slot], w_sem.at[slot])

    def split_tiles(lo, hi):
        step = 4 * 256
        flat = raw.reshape(2, 2 * depth, 128)

        @pl.loop(lo, hi)
        def _(i):
            slot = lax.rem(i, 2)
            raw_load(i, slot).wait()

            @pl.when(i >= 2)
            def _():
                put_store(i - 2, slot).wait()

            @pl.loop(0, 2 * depth // step)
            def _(p):
                for q in range(4):
                    f32s[q] = flat[slot, pl.ds(pl.multiple_of(p * step + q * 256, 256), 256)].astype(F32)
                for q in range(4):
                    dst = pl.ds(pl.multiple_of(p * (step // 2) + q * 128, 128), 128)
                    for k in range(2):
                        wbuf[slot, 0, k, dst] = f32s[q, pl.ds(k, 128, stride=2)].astype(BF16)

            @pl.when(i + 2 < n_tile)
            def _():
                raw_load(i + 2, slot).start()
            put_store(i, slot).start()

    def up_chunks(h, lo, hi):
        @pl.loop(lo, hi)
        def _(c):
            slot = lax.rem(c, 2)
            up_load(c, slot).wait()
            res = []
            for k in range(2):
                w = jnp.concatenate([wbuf[slot, 0, k], wbuf[slot, 1, k]], axis=-1)
                res.append(jnp.dot(nfull[h], w, preferred_element_type=F32).astype(BF16).astype(F32))
            act[:, pl.ds(pl.multiple_of(c * 256, 256), 256)] = (jax.nn.silu(res[1]) * res[0]).astype(BF16)

            @pl.when(c + 2 < n_up)
            def _():
                up_load(c + 2, slot).start()

    def down_group(h, g):
        for q in range(2):
            c = 2 * g + q
            wd_load(c, q).wait()
            part[h, g, :, q * SUB:(q + 1) * SUB] = jnp.dot(act[...], dbuf[q], preferred_element_type=F32)

            @pl.when(c + 2 < n_down)
            def _():
                wd_load(c + 2, q).start()
        send_s1(1, h, g)

    def write_out(h):
        for j in range(tp_size):
            row = h * rows + lax.rem(me + j, tp_size) * blk
            yield pltpu.make_async_copy(nfull.at[h, pl.ds(j * blk, blk)], out_hbm.at[pl.ds(pl.multiple_of(row, blk), blk)], out_sem.at[h, j])

    for slot in range(2):
        wo_load(slot, slot).start()
        raw_load(slot, slot).start()

    @pl.loop(0, n_grp)
    def _(g):
        for q in range(2):
            c = 2 * g + q
            wo_load(c, q).wait()
            for h in range(2):
                part[h, g, :, q * SUB:(q + 1) * SUB] = jnp.dot(attn[h], dbuf[q, :k_out], preferred_element_type=F32)

            @pl.when(c + 2 < n_down)
            def _():
                wo_load(c + 2, q).start()
        send_s1(0, 0, g)

    for q in range(2):
        wd_load(q, q).start()
    cut = [3, 6, 9, 12, 18, 25, 28]
    done = 0
    for g in range(n_grp):
        split_tiles(done, cut[g])
        done = cut[g]
        ev_s2(0, 0, g)
    send_s1(0, 1, 0)
    split_tiles(done, cut[4])
    ev_final(0, 0)
    send_s1(0, 1, 1)
    split_tiles(cut[4], cut[5])
    ev_ag2(0, 0)
    send_s1(0, 1, 2)
    send_s1(0, 1, 3)
    split_tiles(cut[5], n_tile)
    for i in (n_tile - 2, n_tile - 1):
        put_store(i, i % 2).wait()
    for slot in range(2):
        up_load(slot, slot).start()
    ev_s2(0, 1, 0)
    ev_ag_done(0, 0)
    up_chunks(0, 0, 3)
    ev_s2(0, 1, 1)
    up_chunks(0, 3, 7)
    ev_s2(0, 1, 2)
    up_chunks(0, 7, 12)
    ev_s2(0, 1, 3)
    up_chunks(0, 12, n_up)
    for slot in range(2):
        up_load(slot, slot).start()
    drain(0, 0)
    down_group(0, 0)
    down_group(0, 1)
    ev_final(0, 1)
    down_group(0, 2)
    down_group(0, 3)
    for q in range(2):
        wd_load(q, q).start()
    ev_s2(1, 0, 0)
    ev_ag2(0, 1)
    ev_s2(1, 0, 1)
    ev_ag_done(0, 1)
    up_chunks(1, 0, 2)
    ev_s2(1, 0, 2)
    up_chunks(1, 2, 6)
    ev_s2(1, 0, 3)
    up_chunks(1, 6, n_up)
    drain(0, 1)
    ev_final(1, 0)
    down_group(1, 0)
    down_group(1, 1)
    down_group(1, 2)
    ev_ag2(1, 0)
    down_group(1, 3)
    for g in range(n_grp):
        ev_s2(1, 1, g)
    ev_ag_done(1, 0)
    for copy in write_out(0):
        copy.start()
    ev_final(1, 1)
    ev_ag2(1, 1)
    ev_ag_done(1, 1)
    for copy in write_out(1):
        copy.start()
    drain(1, 0)
    drain(1, 1)
    for h in range(2):
        for copy in write_out(h):
            copy.wait()


def mega(attn, xown, gain, w_out, w_ug, w_down, tp_size):
    halves, rows, k_out = attn.shape
    depth, _, ffn = w_ug.shape
    blk = rows // tp_size
    n_grp = 4
    width = depth // n_grp
    vmem = pl.BlockSpec(memory_space=pltpu.VMEM)
    hbm = pl.BlockSpec(memory_space=pl.ANY)
    dma = pltpu.SemaphoreType.DMA
    out, _ = pl.pallas_call(
        mega_kernel,
        in_specs=[vmem, vmem, vmem, hbm, hbm, hbm],
        out_specs=[hbm, hbm],
        out_shape=[jax.ShapeDtypeStruct((halves * rows, depth), BF16), jax.ShapeDtypeStruct((ffn // 128, 2, depth, 128), BF16)],
        scratch_shapes=[
            pltpu.VMEM((2, n_grp, rows, width), F32),
            pltpu.VMEM((2, 2, 2, n_grp, blk, width), F32),
            pltpu.VMEM((2, 2, 2, n_grp, blk // 2, width), F32),
            pltpu.VMEM((2, rows, depth), BF16),
            pltpu.VMEM((2, blk, depth), BF16),
            pltpu.VMEM((rows, ffn), BF16),
            pltpu.VMEM((2, 2, 2, depth, 128), BF16),
            pltpu.VMEM((2, ffn, SUB), BF16),
            pltpu.VMEM((2, depth, 2, 128), BF16),
            pltpu.VMEM((4, 256, 128), F32),
            dma((2, 2, 2, n_grp)), dma((2, 2, 2, n_grp)), dma((2, 2, 2, n_grp)), dma((2, 2, 2, n_grp)),
            dma((2, 2, 2, 2)), dma((2, 2, 2, 2)),
            dma((2,)), dma((2,)), dma((2,)), dma((2,)), dma((2, tp_size)),
        ],
        compiler_params=pltpu.CompilerParams(collective_id=0, has_side_effects=True, vmem_limit_bytes=62 * 2 ** 20),
        cost_estimate=pl.CostEstimate(flops=6 * halves * rows * depth * ffn, bytes_accessed=4 * depth * ffn * 2, transcendentals=0),
        name='prefill_tail',
    )(attn, xown, gain, w_out, w_ug, w_down)
    return out


def roll_rows(vals, start):
    return lax.dynamic_slice_in_dim(jnp.concatenate([vals, vals]), start, vals.shape[0], axis=0)


def prompt_attention(x_rows, seq_len, w_qkv, head_dim, group, gain, half_len):
    num_rows = x_rows.shape[0]
    kv_loc = w_qkv.shape[1]
    positions = jnp.arange(num_rows)
    normed = rms_norm(x_rows, gain)
    qkv_all = jnp.einsum('sd,dhe->she', normed, w_qkv, preferred_element_type=F32).astype(BF16)
    qkv_all = qkv_all.reshape(num_rows, kv_loc, group + 2, head_dim)
    queries = rope_rot(qkv_all[:, :, :group], positions)
    key_all = rope_rot(qkv_all[:, :, group], positions)
    val_all = qkv_all[:, :, group + 1]
    outs = []
    for q_start in range(0, num_rows, half_len):
        k_end = q_start + half_len
        key_pos = jnp.arange(k_end)
        allowed = (key_pos[None, :] <= positions[q_start:k_end, None]) & (key_pos[None, :] < seq_len)
        scores = jnp.einsum('qhgd,khd->hgqk', queries[q_start:k_end], key_all[:k_end], preferred_element_type=F32) * head_dim ** -0.5
        scores = jnp.where(allowed, scores, -1e30)
        attn_prob = jax.nn.softmax(scores, axis=-1).astype(BF16)
        attn_out = jnp.einsum('hgqk,khd->qhgd', attn_prob, val_all[:k_end], preferred_element_type=F32).astype(BF16)
        outs.append(attn_out.reshape(half_len, kv_loc * group * head_dim))
    valid = (positions < seq_len)[:, None, None]
    zero_val = jnp.zeros((), BF16)
    return outs, jnp.where(valid, key_all, zero_val), jnp.where(valid, val_all, zero_val)


def hand_off(key_cache, val_cache, tp_size, side_size):
    t_idx = lax.axis_index('tp')
    both = jnp.stack([key_cache, val_cache])
    head0, head1 = both[:, :, 0], both[:, :, 1]
    low = t_idx < tp_size // 2
    received = []
    for rnd in range(2):
        piece = jnp.where(low, head1, head0) if rnd else jnp.where(low, head0, head1)
        pairs = []
        for t in range(tp_size):
            for s in range(side_size):
                dst_t = (t % 2) * 2 + (rnd + t // 2) % 2
                pairs.append((t * side_size + s, dst_t * side_size + (s + side_size // 2) % side_size))
        received.append(lax.ppermute(piece, ('tp', 'side'), pairs))
    even = t_idx % 2 == 0
    slot0 = jnp.where(even, received[0], received[1])
    slot1 = jnp.where(even, received[1], received[0])
    out = jnp.stack([slot0, slot1], axis=2)
    return out[0][None, :, :, None], out[1][None, :, :, None]


def cache_kernel(len_ref, kc_ref, vc_ref, kn_ref, vn_ref, ko_ref, vo_ref):
    slot = len_ref[pl.program_id(0)]
    ko_ref[...] = kc_ref[...]
    vo_ref[...] = vc_ref[...]
    ko_ref[0, pl.ds(slot, 1)] = kn_ref[...]
    vo_ref[0, pl.ds(slot, 1)] = vn_ref[...]


def cache_update(lengths, k_cache, v_cache, key_new, val_new):
    rows, slots, kv_loc, dim = k_cache.shape
    big = pl.BlockSpec((1, slots, kv_loc, dim), lambda b, lens: (b, 0, 0, 0))
    small = pl.BlockSpec((1, kv_loc, dim), lambda b, lens: (b, 0, 0))
    shape = jax.ShapeDtypeStruct(k_cache.shape, k_cache.dtype)
    return pl.pallas_call(
        cache_kernel,
        grid_spec=pltpu.PrefetchScalarGridSpec(num_scalar_prefetch=1, grid=(rows,), in_specs=[big, big, small, small], out_specs=[big, big]),
        out_shape=[shape, shape],
        cost_estimate=pl.CostEstimate(flops=10 ** 9, bytes_accessed=4 * k_cache.size * 2, transcendentals=0),
        name='cache_update',
    )(lengths, k_cache, v_cache, key_new, val_new)


def decode_side(tokens, lengths, k_cache, v_cache, w_qkv, w_out, w_ug, w_down, gains):
    batch_rows = tokens.shape[0]
    kv_loc = w_qkv.shape[1]
    head_dim = (w_qkv.shape[2] - w_out.shape[1]) // 2
    group = w_out.shape[1] // head_dim
    visible = (jnp.arange(k_cache.shape[1])[None, :] <= lengths[:, None])[:, None, None, :]
    normed = rms_norm(tokens, gains[0])
    qkv_all = jnp.einsum('bd,die->bie', normed, w_qkv, preferred_element_type=F32).astype(BF16)
    qkv_all = qkv_all.reshape(batch_rows, kv_loc, group + 2, head_dim)
    queries = rope_rot(qkv_all[:, :, :group], lengths)
    key_new = rope_rot(qkv_all[:, :, group], lengths)
    val_new = qkv_all[:, :, group + 1]
    key_upd, val_upd = cache_update(lengths, k_cache, v_cache, key_new, val_new)
    scores = jnp.einsum('bige,bsie->bigs', queries, key_upd, preferred_element_type=F32) * head_dim ** -0.5
    scores = jnp.where(visible, scores, -1e30)
    attn_prob = jax.nn.softmax(scores, axis=-1).astype(BF16)
    attn_out = jnp.einsum('bigs,bsie->bige', attn_prob, val_upd, preferred_element_type=F32).astype(BF16)
    attn_proj = lax.psum(jnp.einsum('bif,ifd->bd', attn_out.reshape(batch_rows, kv_loc, group * head_dim), w_out, preferred_element_type=F32), 'tp')
    hidden = residual(tokens, attn_proj)
    act = up_act(rms_norm(hidden, gains[1]), w_ug)
    hidden = residual(hidden, lax.psum(jnp.dot(act, w_down, preferred_element_type=F32), 'tp'))
    return hidden, key_upd, val_upd


def solution(mesh):
    tp_size = mesh.shape['tp']
    side_size = mesh.shape['side']
    rows_spec = P(('pair', 'side'), None)
    flat_spec = P(('pair', 'side'))
    cache_spec = P(None, ('pair', 'side'), None, None, 'tp', None)
    prompt_spec = P(None, ('pair', 'side'), None, 'tp', None)
    in_specs = (rows_spec, flat_spec, rows_spec, cache_spec, cache_spec, flat_spec,
                P(None, None, 'tp', None), P(None, 'tp', None, None), P(None, None, None, 'tp'), P(None, 'tp', None), P(),
                P(None, None, None, 'tp', None), P(None, None, 'tp', None, None), P(None, None, None, 'tp'), P(None, 'tp', None), P())
    out_specs = (rows_spec, rows_spec, prompt_spec, prompt_spec, cache_spec, cache_spec)

    def body(x_prompt, s_len, y_tok, k_cache, v_cache, c_len, wqkv_a, wo_a, wug_a, wd_a, norm_a, wqkv_b, wo_b, wug_b, wd_b, norm_b):
        t_idx = lax.axis_index('tp')
        half_len = x_prompt.shape[0] // 2
        blk = half_len // tp_size
        head_dim = (wqkv_a.shape[3] - wo_a.shape[2]) // 2
        group = wo_a.shape[2] // head_dim
        w_out = wo_a[0].reshape(-1, wo_a.shape[3])
        attn, key_cache, val_cache = prompt_attention(x_prompt, s_len[0], wqkv_a[0], head_dim, group, norm_a[0, 0], half_len)
        rolled = jnp.stack([roll_rows(part, t_idx * blk) for part in attn])
        own = jnp.stack([lax.dynamic_slice_in_dim(x_prompt, idx * half_len + t_idx * blk, blk, axis=0) for idx in range(2)])
        k_prompt, v_prompt = hand_off(key_cache, val_cache, tp_size, side_size)
        hidden = mega(rolled, own, norm_a[0, 1:2], w_out, wug_a[0], wd_a[0], tp_size)
        kc = k_cache[0, :, :, :, 0]
        vc = v_cache[0, :, :, :, 0]
        y_out, k_new, v_new = decode_side(y_tok, c_len, kc, vc, wqkv_b[0, :, :, 0], wo_b[0, :, 0], wug_b[0], wd_b[0], norm_b[0])
        return hidden, y_out, k_prompt, v_prompt, k_new[None, :, :, :, None], v_new[None, :, :, :, None]

    return jax.shard_map(body, mesh=mesh, in_specs=in_specs, out_specs=out_specs, check_vma=False)
```

```python
import functools

import jax
import jax.numpy as jnp
from jax import lax
from jax.experimental import pallas as pl
from jax.experimental.pallas import tpu as pltpu
from jax.sharding import PartitionSpec as P

ROPE_BASE = 10000.0
NORM_EPS = 1e-5
F32 = jnp.float32
BF16 = jnp.bfloat16


def rms_norm(hidden, gain):
    val_f32 = hidden.astype(F32)
    inv_rms = lax.rsqrt(jnp.mean(val_f32 * val_f32, axis=-1, keepdims=True) + NORM_EPS)
    return (val_f32 * inv_rms * gain.astype(F32)).astype(BF16)


def rope_rot(vals_in, positions):
    half_dim = vals_in.shape[-1] // 2
    inv_freq = ROPE_BASE ** (-jnp.arange(half_dim, dtype=F32) / half_dim)
    angles = positions.astype(F32)[:, None] * inv_freq[None, :]
    tab_shape = (angles.shape[0],) + (1,) * (vals_in.ndim - 2) + (half_dim,)
    cos_tab = jnp.cos(angles).reshape(tab_shape)
    sin_tab = jnp.sin(angles).reshape(tab_shape)
    lo_half = vals_in[..., :half_dim].astype(F32)
    hi_half = vals_in[..., half_dim:].astype(F32)
    return jnp.concatenate([lo_half * cos_tab - hi_half * sin_tab, hi_half * cos_tab + lo_half * sin_tab], axis=-1).astype(BF16)


MESH = pl.DeviceIdType.MESH
BOTH = tuple(range(2))
OUT, FFN = BOTH
FIRST, SECOND = BOTH
SUB = 512


def mega_kernel(attn, xown, gain, wo_hbm, wug_hbm, wd_hbm, dattn, tok, dgain, dwo_hbm, dwug_hbm, dwd_hbm, out_hbm, dense_hbm, y_out,
                part, r1, r2, nfull, hown, act, wbuf, dbuf, raw, f32s, dx, dh, dlhs, dact,
                s1_send, s1_recv, s2_send, s2_recv, ag_send, ag_recv,
                w_sem, d_sem, raw_sem, put_sem, out_sem, dx_send, dx_recv):
    tp_size = lax.axis_size('tp')
    me = lax.axis_index('tp')
    right, left = lax.rem(me + 1, tp_size), lax.rem(me + tp_size - 1, tp_size)
    _, n_grp, rows, width = part.shape
    blk = rows // tp_size
    half = blk // 2
    depth = wug_hbm.shape[0]
    n_tile = dense_hbm.shape[0]
    n_up = n_tile // 2
    n_down = wd_hbm.shape[1] // SUB
    n_dec = tok.shape[0]
    k_out = wo_hbm.shape[0]
    peers = (right, left)

    barrier = pltpu.get_barrier_semaphore()
    for step in range(1, tp_size):
        pl.semaphore_signal(barrier, inc=1, device_id={'tp': lax.rem(me + step, tp_size)}, device_id_type=MESH)
    pl.semaphore_wait(barrier, tp_size - 1)

    def remote(src, dst, send, recv, way):
        return pltpu.make_async_remote_copy(src_ref=src, dst_ref=dst, send_sem=send, recv_sem=recv,
                                            device_id={'tp': peers[way]}, device_id_type=MESH)

    def s1_copy(st, h, g, way):
        src = part.at[h, g, pl.ds(blk + half + way * blk, blk)]
        return remote(src, r1.at[st, h, way, g], s1_send.at[st, h, way, g], s1_recv.at[st, h, way, g], way)

    def s2_copy(st, h, g, way):
        src = part.at[h, g, pl.ds(blk if way == 0 else 3 * blk + half, half)]
        return remote(src, r2.at[st, h, way, g], s2_send.at[st, h, way, g], s2_recv.at[st, h, way, g], way)

    def ag1_copy(st, h, way):
        return remote(nfull.at[h, pl.ds(0, blk)], nfull.at[h, pl.ds(3 * blk if way == 0 else blk, blk)],
                      ag_send.at[st, h, way, 0], ag_recv.at[st, h, way, 0], way)

    def ag2_copy(st, h, way):
        src = nfull.at[h, pl.ds(3 * blk if way == 0 else blk + half, half)]
        return remote(src, nfull.at[h, pl.ds(2 * blk + way * half, half)],
                      ag_send.at[st, h, way, 1], ag_recv.at[st, h, way, 1], way)

    def send_s1(st, h, g):
        for way in BOTH:
            s1_copy(st, h, g, way).start()

    def ev_s2(st, h, g):
        for way in BOTH:
            s1_copy(st, h, g, way).wait_recv()
        part[h, g, blk:blk + half] += r1[st, h, 0, g, half:]
        s2_copy(st, h, g, 0).start()
        part[h, g, 3 * blk + half:] += r1[st, h, 1, g, :half]
        s2_copy(st, h, g, 1).start()

    def ev_final(st, h):
        for g in range(n_grp):
            for way in BOTH:
                s2_copy(st, h, g, way).wait_recv()
            cols = slice(g * width, (g + 1) * width)
            base = xown if st == OUT else hown
            top = part[h, g, :half] + (r1[st, h, 1, g, half:] + r2[st, h, 0, g])
            bot = part[h, g, half:blk] + (r1[st, h, 0, g, :half] + r2[st, h, 1, g])
            total = jnp.concatenate([top, bot], axis=0).astype(BF16)
            new = (base[h, :, cols].astype(F32) + total.astype(F32)).astype(BF16)
            if st == OUT:
                hown[h, :, cols] = new
            else:
                nfull[h, :blk, cols] = new
        if st == OUT:
            for r in range(0, blk, 16):
                val = hown[h, r:r + 16].astype(F32)
                inv = lax.rsqrt(jnp.mean(val * val, axis=-1, keepdims=True) + NORM_EPS)
                nfull[h, r:r + 16] = (val * inv * gain[...].astype(F32)).astype(BF16)
        for way in BOTH:
            ag1_copy(st, h, way).start()

    def ev_ag2(st, h):
        for way in BOTH:
            ag1_copy(st, h, way).wait_recv()
            ag2_copy(st, h, way).start()

    def ev_ag_done(st, h):
        for way in BOTH:
            ag2_copy(st, h, way).wait_recv()

    def drain(st, h):
        for way in BOTH:
            for g in range(n_grp):
                s1_copy(st, h, g, way).wait_send()
                s2_copy(st, h, g, way).wait_send()
            ag1_copy(st, h, way).wait_send()
            ag2_copy(st, h, way).wait_send()

    def wo_load(c, slot, src=wo_hbm):
        return pltpu.make_async_copy(src.at[:, pl.ds(pl.multiple_of(c * SUB, SUB), SUB)], dbuf.at[slot, pl.ds(0, k_out)], d_sem.at[slot])

    def wd_load(c, slot, src=wd_hbm):
        return pltpu.make_async_copy(src.at[:, pl.ds(pl.multiple_of(c * SUB, SUB), SUB)], dbuf.at[slot], d_sem.at[slot])

    def raw_load(i, slot, src=wug_hbm):
        return pltpu.make_async_copy(src.at[:, :, pl.ds(pl.multiple_of(i * 128, 128), 128)], raw.at[slot], raw_sem.at[slot])

    def put_store(i, slot):
        return pltpu.make_async_copy(wbuf.at[slot, 0], dense_hbm.at[i], put_sem.at[slot])

    def up_load(c, slot):
        return pltpu.make_async_copy(dense_hbm.at[pl.ds(2 * c, 2)], wbuf.at[slot], w_sem.at[slot])

    def split_tiles(lo, hi):
        step = 4 * 256
        flat = raw.reshape(4, 2 * depth, 128)

        @pl.loop(lo, hi)
        def _(i):
            slot = lax.rem(i, 2)
            raw_load(i, slot).wait()

            @pl.when(i >= 2)
            def _():
                put_store(i - 2, slot).wait()

            @pl.loop(0, 2 * depth // step)
            def _(p):
                for q in range(4):
                    f32s[q] = flat[slot, pl.ds(pl.multiple_of(p * step + q * 256, 256), 256)].astype(F32)
                for q in range(4):
                    dst = pl.ds(pl.multiple_of(p * (step // 2) + q * 128, 128), 128)
                    for k in BOTH:
                        wbuf[slot, 0, k, dst] = f32s[q, pl.ds(k, 128, stride=2)].astype(BF16)

            @pl.when(i + 2 < n_tile)
            def _():
                raw_load(i + 2, slot).start()
            put_store(i, slot).start()

    def up_chunks(h, lo, hi):
        @pl.loop(lo, hi)
        def _(c):
            slot = lax.rem(c, 2)
            up_load(c, slot).wait()
            res = []
            for k in BOTH:
                w = jnp.concatenate([wbuf[slot, 0, k], wbuf[slot, 1, k]], axis=-1)
                res.append(jnp.dot(nfull[h], w, preferred_element_type=F32).astype(BF16).astype(F32))
            act[:, pl.ds(pl.multiple_of(c * 256, 256), 256)] = (jax.nn.silu(res[1]) * res[0]).astype(BF16)

            @pl.when(c + 2 < n_up)
            def _():
                up_load(c + 2, slot).start()

    def down_group(h, g):
        for q in BOTH:
            c = 2 * g + q
            wd_load(c, q).wait()
            part[h, g, :, q * SUB:(q + 1) * SUB] = jnp.dot(act[...], dbuf[q], preferred_element_type=F32)

            @pl.when(c + 2 < n_down)
            def _():
                wd_load(c + 2, q).start()

    def write_out(h):
        for j in range(tp_size):
            row = h * rows + lax.rem(me + j, tp_size) * blk
            yield pltpu.make_async_copy(nfull.at[h, pl.ds(j * blk, blk)], out_hbm.at[pl.ds(pl.multiple_of(row, blk), blk)], out_sem.at[h, j])

    def dx_copy(st, step):
        return pltpu.make_async_remote_copy(src_ref=dx.at[st, me], dst_ref=dx.at[st, me], send_sem=dx_send.at[st, step - 1], recv_sem=dx_recv.at[st, step - 1],
                                            device_id={'tp': lax.rem(me + step, tp_size)}, device_id_type=MESH)

    def dx_start(st):
        for step in range(1, tp_size):
            dx_copy(st, step).start()

    def dx_total(st):
        for step in range(1, tp_size):
            dx_copy(st, step).wait_recv()
        total = dx[st, 0]
        for src in range(1, tp_size):
            total = total + dx[st, src]
        return total.astype(BF16).astype(F32)

    def dec_out():
        @pl.loop(0, n_grp)
        def _(g):
            for q in BOTH:
                c = 2 * g + q
                wo_load(c, q, dwo_hbm).wait()
                dx[0, me, :, pl.ds(pl.multiple_of(c * SUB, SUB), SUB)] = jnp.dot(dattn[...], dbuf[q, :k_out], preferred_element_type=F32)

                @pl.when(c + 2 < n_down)
                def _():
                    wo_load(c + 2, q, dwo_hbm).start()
        dx_start(0)

    def dec_norm():
        hid = (tok[...].astype(F32) + dx_total(0)).astype(BF16)
        dh[...] = hid
        val = hid.astype(F32)
        inv = lax.rsqrt(jnp.mean(val * val, axis=-1, keepdims=True) + NORM_EPS)
        normed = (val * inv * dgain[...].astype(F32)).astype(BF16)
        row = lax.broadcasted_iota(jnp.int32, (256, SUB), 0)
        col = lax.broadcasted_iota(jnp.int32, (256, SUB), 1)
        for k in BOTH:
            spread = (col == 2 * row + k).astype(F32).astype(BF16)
            for c in range(depth // 256):
                piece = jnp.dot(normed[:, c * 256:(c + 1) * 256], spread, preferred_element_type=F32)
                dlhs[k * n_dec:(k + 1) * n_dec, c * SUB:(c + 1) * SUB] = piece

    def dec_up(lo, hi):
        flat = raw.reshape(4, 2 * depth, 128)

        @pl.loop(lo, hi)
        def _(c):
            pair = 2 * lax.rem(c, 2)
            for q in BOTH:
                raw_load(2 * c + q, pair + q, dwug_hbm).wait()
            w = jnp.concatenate([flat[pair], flat[pair + 1]], axis=-1)
            res = jnp.dot(dlhs[...].astype(BF16), w, preferred_element_type=F32).astype(BF16).astype(F32)
            dact[:, pl.ds(pl.multiple_of(c * 256, 256), 256)] = jax.nn.silu(res[n_dec:]) * res[:n_dec]

            @pl.when(c + 2 < n_up)
            def _():
                for q in BOTH:
                    raw_load(2 * c + 4 + q, pair + q, dwug_hbm).start()

    def dec_down(lo, hi):
        @pl.loop(lo, hi)
        def _(g):
            for q in BOTH:
                c = 2 * g + q
                wd_load(c, q, dwd_hbm).wait()
                dx[1, me, :, pl.ds(pl.multiple_of(c * SUB, SUB), SUB)] = jnp.dot(dact[...].astype(BF16), dbuf[q], preferred_element_type=F32)

                @pl.when(c + 2 < n_down)
                def _():
                    wd_load(c + 2, q, dwd_hbm).start()

    for slot in BOTH:
        wo_load(slot, slot).start()
        raw_load(slot, slot).start()

    @pl.loop(0, n_grp)
    def _(g):
        for q in BOTH:
            c = 2 * g + q
            wo_load(c, q).wait()
            for h in BOTH:
                part[h, g, :, q * SUB:(q + 1) * SUB] = jnp.dot(attn[h], dbuf[q, :k_out], preferred_element_type=F32)

            @pl.when(c + 2 < n_down)
            def _():
                wo_load(c + 2, q).start()
        send_s1(OUT, FIRST, g)

    for q in BOTH:
        wo_load(q, q, dwo_hbm).start()
    dec_out()
    for q in BOTH:
        wd_load(q, q).start()
    cut = [3, 6, 9, 12, 18, 25, 28]
    done = 0
    for g in range(n_grp):
        split_tiles(done, cut[g])
        done = cut[g]
        ev_s2(OUT, FIRST, g)
    send_s1(OUT, SECOND, 0)
    split_tiles(done, cut[4])
    ev_final(OUT, FIRST)
    send_s1(OUT, SECOND, 1)
    split_tiles(cut[4], cut[5])
    ev_ag2(OUT, FIRST)
    send_s1(OUT, SECOND, 2)
    send_s1(OUT, SECOND, 3)
    split_tiles(cut[5], n_tile)
    for i in (n_tile - 2, n_tile - 1):
        put_store(i, i % 2).wait()
    for slot in BOTH:
        up_load(slot, slot).start()
    ev_s2(OUT, SECOND, 0)
    ev_ag_done(OUT, FIRST)
    up_chunks(FIRST, 0, 3)
    ev_s2(OUT, SECOND, 1)
    up_chunks(FIRST, 3, 7)
    ev_s2(OUT, SECOND, 2)
    up_chunks(FIRST, 7, 12)
    ev_s2(OUT, SECOND, 3)
    up_chunks(FIRST, 12, n_up)
    for slot in BOTH:
        up_load(slot, slot).start()
    drain(OUT, FIRST)
    for i in range(4):
        raw_load(i, i, dwug_hbm).start()
    down_group(FIRST, 0)
    down_group(FIRST, 1)
    ev_final(OUT, SECOND)
    send_s1(FFN, FIRST, 0)
    down_group(FIRST, 2)
    down_group(FIRST, 3)
    for q in BOTH:
        wd_load(q, q).start()
    dec_norm()
    dec_up(0, 3)
    ev_ag2(OUT, SECOND)
    for g in range(1, n_grp):
        send_s1(FFN, FIRST, g)
    dec_up(3, 9)
    ev_s2(FFN, FIRST, 0)
    ev_ag_done(OUT, SECOND)
    up_chunks(SECOND, 0, 5)
    ev_s2(FFN, FIRST, 1)
    up_chunks(SECOND, 5, 9)
    ev_s2(FFN, FIRST, 2)
    up_chunks(SECOND, 9, n_up)
    ev_s2(FFN, FIRST, 3)
    drain(OUT, SECOND)
    for g in range(n_grp):
        down_group(SECOND, g)
        send_s1(FFN, SECOND, g)
    for q in BOTH:
        wd_load(q, q, dwd_hbm).start()
    dec_up(9, n_up)
    ev_s2(FFN, SECOND, 0)
    ev_s2(FFN, SECOND, 1)
    dec_down(0, 2)
    ev_s2(FFN, SECOND, 2)
    dec_down(2, n_grp)
    dx_start(1)
    ev_s2(FFN, SECOND, 3)
    ev_final(FFN, FIRST)
    ev_final(FFN, SECOND)
    ev_ag2(FFN, FIRST)
    ev_ag2(FFN, SECOND)
    ev_ag_done(FFN, FIRST)
    for copy in write_out(0):
        copy.start()
    ev_ag_done(FFN, SECOND)
    for copy in write_out(1):
        copy.start()
    y_out[...] = (dh[...].astype(F32) + dx_total(1)).astype(BF16)
    for st in BOTH:
        for step in range(1, tp_size):
            dx_copy(st, step).wait_send()
    drain(FFN, FIRST)
    drain(FFN, SECOND)
    for h in BOTH:
        for copy in write_out(h):
            copy.wait()


def mega(attn, xown, gain, w_out, w_ug, w_down, dattn, tok, dgain, dw_out, dw_ug, dw_down, tp_size):
    halves, rows, k_out = attn.shape
    depth, _, ffn = w_ug.shape
    blk = rows // tp_size
    n_grp = 4
    width = depth // n_grp
    vmem = pl.BlockSpec(memory_space=pltpu.VMEM)
    hbm = pl.BlockSpec(memory_space=pl.ANY)
    dma = pltpu.SemaphoreType.DMA
    trio = (2,) * 3
    n_dec = tok.shape[0]
    out, _, y_out = pl.pallas_call(
        mega_kernel,
        in_specs=[vmem, vmem, vmem, hbm, hbm, hbm] * 2,
        out_specs=[hbm, hbm, vmem],
        out_shape=[jax.ShapeDtypeStruct((halves * rows, depth), BF16), jax.ShapeDtypeStruct((ffn // 128, 2, depth, 128), BF16), jax.ShapeDtypeStruct(tok.shape, BF16)],
        scratch_shapes=[
            pltpu.VMEM((2, n_grp, rows, width), F32),
            pltpu.VMEM((*trio, n_grp, blk, width), F32),
            pltpu.VMEM((*trio, n_grp, blk // 2, width), F32),
            pltpu.VMEM((2, rows, depth), BF16),
            pltpu.VMEM((2, blk, depth), BF16),
            pltpu.VMEM((rows, ffn), BF16),
            pltpu.VMEM((*trio, depth, 128), BF16),
            pltpu.VMEM((2, ffn, SUB), BF16),
            pltpu.VMEM((4, depth, 2, 128), BF16),
            pltpu.VMEM((4, 256, 128), F32),
            pltpu.VMEM((2, tp_size, n_dec, depth), F32),
            pltpu.VMEM((n_dec, depth), BF16),
            pltpu.VMEM((2 * n_dec, 2 * depth), F32),
            pltpu.VMEM((n_dec, ffn), F32),
            *[dma((*trio, n_grp))] * 4, *[dma((*trio, 2))] * 2,
            *[dma((4,))] * 4, *[dma((2, tp_size))] * 3,
        ],
        compiler_params=pltpu.CompilerParams(collective_id=0, has_side_effects=True, vmem_limit_bytes=62 * 2 ** 20),
        cost_estimate=pl.CostEstimate(flops=6 * halves * rows * depth * ffn, bytes_accessed=4 * depth * ffn * 2, transcendentals=0),
        name='prefill_tail',
    )(attn, xown, gain, w_out, w_ug, w_down, dattn, tok, dgain, dw_out, dw_ug, dw_down)
    return out, y_out


def prompt_kernel(meta, qkv, cos, sin, out, kv_out, *, group, dim, tp_size):
    seq_len, me = meta[0], meta[1]
    rows = qkv.shape[1]
    half_len = rows // 2
    blk = half_len // tp_size

    def rope(col, lo, hi):
        val = qkv[0, lo:hi, col * dim:(col + 1) * dim].astype(F32)
        return (val * cos[lo:hi] + pltpu.roll(val, dim // 2, 1) * sin[lo:hi]).astype(BF16)

    keys = rope(group, 0, rows)
    vals = qkv[0, :, (group + 1) * dim:]
    valid = lax.broadcasted_iota(jnp.int32, (rows, dim), 0) < seq_len
    kv_out[0, 0] = jnp.where(valid, keys.astype(F32), 0.0).astype(BF16)
    kv_out[0, 1] = jnp.where(valid, vals.astype(F32), 0.0).astype(BF16)
    for idx in BOTH:
        lo, hi = idx * half_len, (idx + 1) * half_len
        key_pos = lax.broadcasted_iota(jnp.int32, (half_len, hi), 1)
        query_pos = lax.broadcasted_iota(jnp.int32, (half_len, hi), 0) + lo
        allowed = (key_pos <= query_pos) & (key_pos < seq_len)
        for g in range(group):
            query = rope(g, lo, hi)
            scores = lax.dot_general(query, keys[:hi], (((1,), (1,)), ((), ())), preferred_element_type=F32) * dim ** -0.5
            scores = jnp.where(allowed, scores, -1e30)
            expo = jnp.exp(scores - jnp.max(scores, axis=-1, keepdims=True))
            prob = (expo / jnp.sum(expo, axis=-1, keepdims=True)).astype(BF16)
            res = jnp.dot(prob, vals[:hi], preferred_element_type=F32).astype(BF16)
            for b in range(tp_size):
                slot = lax.rem(b + tp_size - me, tp_size)
                out[idx, pl.ds(pl.multiple_of(slot * blk, blk), blk), g * dim:(g + 1) * dim] = res[b * blk:(b + 1) * blk]


def prompt_attention(x_rows, seq_len, w_qkv, head_dim, group, gain, tp_size):
    num_rows = x_rows.shape[0]
    kv_loc = w_qkv.shape[1]
    t_idx = lax.axis_index('tp')
    normed = rms_norm(x_rows, gain)
    qkv_all = jnp.einsum('sd,dhe->hse', normed, w_qkv, preferred_element_type=F32).astype(BF16)
    half_dim = head_dim // 2
    inv_freq = ROPE_BASE ** (-jnp.arange(half_dim, dtype=F32) / half_dim)
    angles = jnp.arange(num_rows).astype(F32)[:, None] * inv_freq[None, :]
    cos_tab = jnp.cos(angles)
    sin_tab = jnp.sin(angles)
    cos_tab = jnp.concatenate([cos_tab, cos_tab], axis=-1)
    sin_tab = jnp.concatenate([-sin_tab, sin_tab], axis=-1)
    table = pl.BlockSpec((num_rows, head_dim), lambda h, meta: (0, 0))
    width = group * head_dim
    return pl.pallas_call(
        functools.partial(prompt_kernel, group=group, dim=head_dim, tp_size=tp_size),
        grid_spec=pltpu.PrefetchScalarGridSpec(
            num_scalar_prefetch=1, grid=(kv_loc,),
            in_specs=[pl.BlockSpec((1, num_rows, w_qkv.shape[2]), lambda h, meta: (h, 0, 0)), table, table],
            out_specs=[pl.BlockSpec((2, num_rows // 2, width), lambda h, meta: (0, 0, h)),
                       pl.BlockSpec((1, 2, num_rows, head_dim), lambda h, meta: (lax.rem(h + meta[1] // (tp_size // kv_loc), kv_loc), 0, 0, 0))]),
        out_shape=[jax.ShapeDtypeStruct((2, num_rows // 2, kv_loc * width), BF16),
                   jax.ShapeDtypeStruct((kv_loc, 2, num_rows, head_dim), BF16)],
        cost_estimate=pl.CostEstimate(flops=4 * num_rows * num_rows * kv_loc * width, bytes_accessed=2 ** 22, transcendentals=num_rows * num_rows * kv_loc * group),
        name='prompt_attention',
    )(jnp.stack([seq_len, t_idx.astype(jnp.int32)]), qkv_all, cos_tab, sin_tab)


def hand_off(pieces, tp_size, side_size):
    t_idx = lax.axis_index('tp')
    received = []
    for rnd in BOTH:
        pairs = []
        for t in range(tp_size):
            for s in range(side_size):
                dst_t = (t % 2) * 2 + (rnd + t // 2) % 2
                pairs.append((t * side_size + s, dst_t * side_size + (s + side_size // 2) % side_size))
        received.append(lax.ppermute(pieces[rnd], ('tp', 'side'), pairs))
    even = t_idx % 2 == 0
    slot0 = jnp.where(even, received[0], received[1])
    slot1 = jnp.where(even, received[1], received[0])
    out = jnp.stack([slot0, slot1], axis=2)
    return out[0][None, :, :, None], out[1][None, :, :, None]


def cache_kernel(len_ref, kc_ref, vc_ref, kn_ref, vn_ref, ko_ref, vo_ref):
    slot = len_ref[pl.program_id(0)]
    ko_ref[...] = kc_ref[...]
    vo_ref[...] = vc_ref[...]
    ko_ref[0, pl.ds(slot, 1)] = kn_ref[...]
    vo_ref[0, pl.ds(slot, 1)] = vn_ref[...]


def cache_update(lengths, k_cache, v_cache, key_new, val_new):
    rows, slots, kv_loc, dim = k_cache.shape
    big = pl.BlockSpec((1, slots, kv_loc, dim), lambda b, lens: (b, 0, 0, 0))
    small = pl.BlockSpec((1, kv_loc, dim), lambda b, lens: (b, 0, 0))
    shape = jax.ShapeDtypeStruct(k_cache.shape, k_cache.dtype)
    return pl.pallas_call(
        cache_kernel,
        grid_spec=pltpu.PrefetchScalarGridSpec(num_scalar_prefetch=1, grid=(rows,), in_specs=[big, big, small, small], out_specs=[big, big]),
        out_shape=[shape, shape],
        cost_estimate=pl.CostEstimate(flops=10 ** 9, bytes_accessed=4 * k_cache.size * 2, transcendentals=0),
        name='cache_update',
    )(lengths, k_cache, v_cache, key_new, val_new)


def decode_attention(tokens, lengths, k_cache, v_cache, w_qkv, head_dim, group, gain):
    batch_rows = tokens.shape[0]
    kv_loc = w_qkv.shape[1]
    visible = (jnp.arange(k_cache.shape[1])[None, :] <= lengths[:, None])[:, None, None, :]
    normed = rms_norm(tokens, gain)
    qkv_all = jnp.einsum('bd,die->bie', normed, w_qkv, preferred_element_type=F32).astype(BF16)
    qkv_all = qkv_all.reshape(batch_rows, kv_loc, group + 2, head_dim)
    queries = rope_rot(qkv_all[:, :, :group], lengths)
    key_new = rope_rot(qkv_all[:, :, group], lengths)
    val_new = qkv_all[:, :, group + 1]
    key_upd, val_upd = cache_update(lengths, k_cache, v_cache, key_new, val_new)
    scores = jnp.einsum('bige,bsie->bigs', queries, key_upd, preferred_element_type=F32) * head_dim ** -0.5
    scores = jnp.where(visible, scores, -1e30)
    attn_prob = jax.nn.softmax(scores, axis=-1).astype(BF16)
    attn_out = jnp.einsum('bigs,bsie->bige', attn_prob, val_upd, preferred_element_type=F32).astype(BF16)
    return attn_out.reshape(batch_rows, kv_loc * group * head_dim), key_upd, val_upd


def solution(mesh):
    tp_size = mesh.shape['tp']
    side_size = mesh.shape['side']
    def at_tp(rank, dim):
        return P(*['tp' if i == dim else None for i in range(rank)])

    group_axes = ('pair', 'side')
    rows_spec = P(group_axes, None)
    flat_spec = P(group_axes)
    cache_spec = P(None, group_axes, None, None, 'tp', None)
    prompt_spec = P(None, group_axes, None, 'tp', None)
    wide, tall = at_tp(4, 3), at_tp(3, 1)
    in_specs = (rows_spec, flat_spec, rows_spec, cache_spec, cache_spec, flat_spec,
                at_tp(4, 2), at_tp(4, 1), wide, tall, P(), at_tp(5, 3), at_tp(5, 2), wide, tall, P())
    out_specs = (rows_spec, rows_spec, prompt_spec, prompt_spec, cache_spec, cache_spec)

    def body(x_prompt, s_len, y_tok, k_cache, v_cache, c_len, wqkv_a, wo_a, wug_a, wd_a, norm_a, wqkv_b, wo_b, wug_b, wd_b, norm_b):
        t_idx = lax.axis_index('tp')
        half_len = x_prompt.shape[0] // 2
        blk = half_len // tp_size
        head_dim = (wqkv_a.shape[3] - wo_a.shape[2]) // 2
        group = wo_a.shape[2] // head_dim
        w_out = wo_a[0].reshape(-1, wo_a.shape[3])
        rolled, pieces = prompt_attention(x_prompt, s_len[0], wqkv_a[0], head_dim, group, norm_a[0, 0], tp_size)
        own = jnp.stack([lax.dynamic_slice_in_dim(x_prompt, idx * half_len + t_idx * blk, blk, axis=0) for idx in BOTH])
        k_prompt, v_prompt = hand_off(pieces, tp_size, side_size)
        dattn, k_new, v_new = decode_attention(y_tok, c_len, k_cache[0, :, :, :, 0], v_cache[0, :, :, :, 0], wqkv_b[0, :, :, 0], head_dim, group, norm_b[0, 0])
        hidden, y_out = mega(rolled, own, norm_a[0, 1:2], w_out, wug_a[0], wd_a[0],
                             dattn, y_tok, norm_b[0, 1:2], wo_b[0, :, 0].reshape(w_out.shape), wug_b[0], wd_b[0], tp_size)
        return hidden, y_out, k_prompt, v_prompt, k_new[None, :, :, :, None], v_new[None, :, :, :, None]

    return jax.shard_map(body, mesh=mesh, in_specs=in_specs, out_specs=out_specs, check_vma=False)
```
